32 devices in a mesh: grp: 2 (over x), ha: 16 (over z, y, core).
Axes of the slice: x: 2, y: 2, z: 4, core: 2. Of those that a mesh axis runs over, the one named last changes fastest.
Arguments:
- frames: bfloat16 [4, 16, 112, 384], P('grp', 'ha'), parts along dimension 0, may hold values from -6 to 6
- cache_first: bfloat16 [4, 16, 112, 384], P('grp', 'ha'), parts along dimension 0, may hold values from -5 to 5
- cache_second: bfloat16 [4, 16, 112, 384], P('grp', 'ha'), parts along dimension 0, may hold values from -5 to 5
- gain_first: float32 [384], replicated, may hold values from 0.1 to 1.9
- gain_second: float32 [384], replicated, may hold values from 0.1 to 1.9
- bias_first: float32 [384], replicated, may hold values from -3 to 3
- bias_second: float32 [384], replicated, may hold values from -3 to 3
- weight_first: bfloat16 [10368, 384], P(None, 'ha'), may hold values from -0.0625 to 0.0625
- weight_second: bfloat16 [10368, 384], P(None, 'ha'), may hold values from -0.0625 to 0.0625
- cotangent: bfloat16 [4, 16, 112, 384], P('grp', 'ha'), parts along dimension 0, may hold values from -6 to 6
Outputs:
- output: bfloat16 [4, 16, 112, 384], P('grp', 'ha'), parts along dimension 0
- grad_frames: bfloat16 [4, 16, 112, 384], P('grp', 'ha'), parts along dimension 0
The draws below stay inside these ranges and needn't reach their ends.
There are 2 independent parts, one for each index of `grp`. The reference program is written for one: setup_inputs(seed, part) draws one part's arguments, and reference() takes and returns one part's arrays. A program takes and returns all parts, laid end to end along the dimension named above; an argument that names none is the same for every part. Nothing has to cross between parts.
All inputs are finite; a program needn't handle non-finite values.
Results may differ from the reference program's by a relative error of at most 0.006.
Values may be sent and summed in bfloat16 or wider, within the bound.
No kernel may reach another device: no remote copies, remote signals or barrier semaphores. Data moves between devices by JAX's collectives and lax.ppermute only.
A program may use at most 128 MiB of HBM per device.

```python
import jax
import jax.numpy as jnp
from jax import lax

C = 384
FRAMES = 2
W = 112
H = 16


def level_of(own_key, extent, shards, low, largest):
    def one(axis_at, parts):
        heights = jax.random.uniform(jax.random.fold_in(jax.random.fold_in(own_key, 6), axis_at), (parts,), jnp.float32, low / len(shards), largest / len(shards))
        return jnp.repeat(jnp.exp(heights), extent[axis_at] // parts).reshape((-1,) + (1,) * (len(extent) - axis_at - 1))

    factor_of = one(*shards[0])
    for cut in shards[1:]:
        factor_of = factor_of * one(*cut)
    return factor_of


def noise(own_key, shape, deviation, limit, cuts=(), kind=jnp.bfloat16):
    array = jax.random.normal(own_key, shape, jnp.float32) * deviation
    if len(cuts) > 0:
        array = level_of(own_key, shape, cuts, -0.22, 0.18) * array
    return jnp.clip(array, min=-limit, max=limit).astype(kind)


def setup_inputs(seed: int = 0, part: int = 0) -> dict:
    seeds = jax.random.split(jax.random.key(seed), 11)
    part_splits = jax.random.split(jax.random.fold_in(seeds[10], part), 11)
    return {
        "frames": noise(part_splits[0], (FRAMES, H, W, C), 1.0, 6.0, ((1, 16),)),
        "cache_first": noise(part_splits[1], (2, H, W, C), 0.8, 5.0, ((1, 16),)),
        "cache_second": noise(part_splits[2], (2, H, W, C), 0.8, 5.0, ((1, 16),)),
        "gain_first": jnp.clip(1.0 + 0.18 * jax.random.normal(seeds[3], (C,), jnp.float32), 0.1, 1.9),
        "gain_second": jnp.clip(1.0 + 0.18 * jax.random.normal(seeds[4], (C,), jnp.float32), 0.1, 1.9),
        "bias_first": noise(seeds[5], (C,), 0.5, 3.0, (), jnp.float32),
        "bias_second": noise(seeds[6], (C,), 0.5, 3.0, (), jnp.float32),
        "weight_first": noise(seeds[7], (27 * C, C), (27 * C) ** -0.5, 0.0625, ((1, 16),)),
        "weight_second": noise(seeds[8], (27 * C, C), (27 * C) ** -0.5, 0.0625, ((1, 16),)),
        "cotangent": noise(part_splits[9], (FRAMES, H, W, C), 1.0, 6.0, ((1, 16),)),
    }


def normed_silu(values, scales):
    mean_square = lax.optimization_barrier(jnp.mean(values * values, axis=-1, keepdims=True))
    inverse = lax.rsqrt(mean_square + 1e-06)
    normed = values * inverse * scales
    return normed * jax.nn.sigmoid(normed)

def silu_backward(values, scales, upstream):
    mean_square = lax.optimization_barrier(jnp.mean(values * values, axis=-1, keepdims=True))
    inverse = lax.rsqrt(mean_square + 1e-06)
    normed = values * inverse * scales
    sigmoid_value = jax.nn.sigmoid(normed)
    scaled = scales * upstream * sigmoid_value * (1.0 + normed * (1.0 - sigmoid_value))
    return inverse * scaled - values * inverse ** 3 * lax.optimization_barrier(jnp.mean(values * scaled, axis=-1, keepdims=True))

def conv_forward(extended, weight):
    length = extended.shape[0] - 2
    height, columns, channels = (extended.shape[1], extended.shape[2], extended.shape[3])
    padded = jnp.pad(extended, ((0, 0), (1, 1), (1, 1), (0, 0)))
    kernel = weight.reshape(27, channels, channels)
    summed = jnp.zeros((length * height * columns, channels), jnp.float32)
    for frame_tap in range(3):
        for row_tap in range(3):
            for col_tap in range(3):
                window = padded[frame_tap:frame_tap + length, row_tap:row_tap + height, col_tap:col_tap + columns]
                summed = summed + jnp.dot(window.reshape(-1, channels), kernel[frame_tap * 9 + row_tap * 3 + col_tap], preferred_element_type=jnp.float32)
    return summed.reshape(length, height, columns, channels)

def conv_backward(upstream, weight):
    length, height, columns, channels = upstream.shape
    padded = jnp.pad(upstream, ((0, 2), (1, 1), (1, 1), (0, 0)))
    kernel = weight.reshape(27, channels, channels)
    summed = jnp.zeros((length * height * columns, channels), jnp.float32)
    for frame_tap in range(3):
        for row_tap in range(3):
            for col_tap in range(3):
                window = padded[2 - frame_tap:2 - frame_tap + length, 2 - row_tap:2 - row_tap + height, 2 - col_tap:2 - col_tap + columns]
                summed = summed + jnp.dot(window.reshape(-1, channels), kernel[frame_tap * 9 + row_tap * 3 + col_tap].T, preferred_element_type=jnp.float32)
    return summed.reshape(length, height, columns, channels)

def reference(frames, cache_first, cache_second, gain_first, gain_second, bias_first, bias_second, weight_first, weight_second, cotangent):
    inputs = frames.astype(jnp.float32)
    first_act = normed_silu(inputs, gain_first).astype(jnp.bfloat16)
    middle = (conv_forward(jnp.concatenate([cache_first, first_act], axis=0), weight_first) + bias_first).astype(jnp.bfloat16)
    middle_float = middle.astype(jnp.float32)
    second_act = normed_silu(middle_float, gain_second).astype(jnp.bfloat16)
    second_out = conv_forward(jnp.concatenate([cache_second, second_act], axis=0), weight_second) + bias_second
    output = (inputs + second_out).astype(jnp.bfloat16)
    grad_middle = silu_backward(middle_float, gain_second, conv_backward(cotangent, weight_second)).astype(jnp.bfloat16)
    grad_inputs = silu_backward(inputs, gain_first, conv_backward(grad_middle, weight_first))
    grad_frames = (cotangent.astype(jnp.float32) + grad_inputs).astype(jnp.bfloat16)
    return (output, grad_frames)
```

```python
import jax
import jax.numpy as jnp
from jax import lax
from jax.experimental import pallas as pl
from jax.experimental.pallas import tpu as pltpu
from jax.sharding import PartitionSpec as P

TAPS = 27
SOLE = 10
HALF = SOLE // 2
MID = 4
OWN = HALF + MID
VMEM_LIMIT = 40 * 1024 * 1024


def normed_silu(values, scales):
    mean_square = jnp.mean(values * values, axis=-1, keepdims=True)
    normed = values * lax.rsqrt(mean_square + 1e-06) * scales
    return normed * jax.nn.sigmoid(normed)


def silu_backward(values, scales, upstream):
    mean_square = jnp.mean(values * values, axis=-1, keepdims=True)
    inverse = lax.rsqrt(mean_square + 1e-06)
    normed = values * inverse * scales
    sigmoid_value = jax.nn.sigmoid(normed)
    scaled = scales * upstream * sigmoid_value * (1.0 + normed * (1.0 - sigmoid_value))
    return inverse * scaled - values * inverse**3 * jnp.mean(
        values * scaled, axis=-1, keepdims=True
    )


def shifted(block, by):
    zero = jnp.zeros_like(block[:, :1])
    if by > 0:
        return jnp.concatenate([zero, block[:, :-1]], axis=1)
    return jnp.concatenate([block[:, 1:], zero], axis=1)


def conv_forward(rows_ref, weight_ref, total_ref):
    _, frames, columns, channels = rows_ref.shape
    length = frames - 2
    for col_tap in range(3):
        for frame_tap in range(3):
            for row_tap in range(3):
                tap = 9 * frame_tap + 3 * row_tap + col_tap
                left = rows_ref[row_tap, frame_tap : frame_tap + length]
                product = lax.dot_general(
                    left.reshape(length * columns, channels),
                    weight_ref[:, tap * channels : (tap + 1) * channels],
                    (((1,), (1,)), ((), ())),
                    preferred_element_type=jnp.float32,
                )
                if frame_tap == 0 and row_tap == 0:
                    total_ref[col_tap] = product
                else:
                    total_ref[col_tap] += product
    parts = [total_ref[k].reshape(length, columns, channels) for k in range(3)]
    return shifted(parts[0], 1) + parts[1] + shifted(parts[2], -1)


def conv_backward(rows_ref, weight_ref, total_ref):
    _, length, columns, channels = rows_ref.shape
    for col_tap in range(3):
        for shift in range(min(3, length)):
            frame_tap = 2 - shift
            count = (length - shift) * columns
            for row_tap in range(3):
                tap = 9 * frame_tap + 3 * row_tap + col_tap
                left = rows_ref[2 - row_tap, shift:length]
                product = lax.dot_general(
                    left.reshape(count, channels),
                    weight_ref[:, tap * channels : (tap + 1) * channels],
                    (((1,), (0,)), ((), ())),
                    preferred_element_type=jnp.float32,
                )
                if shift == 0 and row_tap == 0:
                    total_ref[col_tap] = product
                else:
                    total_ref[col_tap, :count] += product
    parts = [total_ref[k].reshape(length, columns, channels) for k in range(3)]
    return shifted(parts[0], -1) + parts[1] + shifted(parts[2], 1)


def first_kernel(
    cache, frames, low, high, gain_first, bias, gain_second, weight, middle, act, rows, total
):
    length = frames.shape[0]
    for row, source in ((0, low), (1, None), (2, high)):
        rows[row, :2] = cache[...] if source is None else source[:2]
        values = frames[...] if source is None else source[2 : 2 + length]
        rows[row, 2:] = normed_silu(values.astype(jnp.float32), gain_first[...]).astype(
            jnp.bfloat16
        )
    result = (conv_forward(rows, weight, total) + bias[...]).astype(jnp.bfloat16)
    middle[...] = result
    act[...] = normed_silu(result.astype(jnp.float32), gain_second[...]).astype(jnp.bfloat16)


def second_kernel(cotangent, low, high, middle, gain, weight, grad, rows, total):
    length = cotangent.shape[0]
    rows[0] = low[2 + length : 2 + 2 * length]
    rows[1] = cotangent[...]
    rows[2] = high[2 + length : 2 + 2 * length]
    upstream = conv_backward(rows, weight, total)
    grad[...] = silu_backward(middle[...].astype(jnp.float32), gain[...], upstream).astype(
        jnp.bfloat16
    )


def third_kernel(cache, act, low, high, act_low, act_high, frames, bias, weight, out, rows, total):
    length = frames.shape[0]
    for row, older, newer in ((0, low, act_low), (1, None, act), (2, high, act_high)):
        rows[row, :2] = cache[...] if older is None else older[2 + 2 * length :]
        rows[row, 2:] = newer[...]
    result = conv_forward(rows, weight, total)
    out[...] = (frames[...].astype(jnp.float32) + result + bias[...]).astype(jnp.bfloat16)


def fourth_kernel(grad, low, high, frames, gain, cotangent, weight, out, rows, total):
    rows[0] = low[...]
    rows[1] = grad[...]
    rows[2] = high[...]
    upstream = conv_backward(rows, weight, total)
    back = silu_backward(frames[...].astype(jnp.float32), gain[...], upstream)
    out[...] = (cotangent[...].astype(jnp.float32) + back).astype(jnp.bfloat16)


def run_kernel(body, frames, outs, operands, dots):
    length, columns, channels = operands[0].shape
    spec = pl.BlockSpec(memory_space=pltpu.VMEM)
    shape = jax.ShapeDtypeStruct((length, columns, channels), jnp.bfloat16)
    return pl.pallas_call(
        body,
        out_shape=[shape] * outs if outs > 1 else shape,
        in_specs=[spec] * len(operands),
        out_specs=[spec] * outs if outs > 1 else spec,
        scratch_shapes=[
            pltpu.VMEM((3, frames, columns, channels), jnp.bfloat16),
            pltpu.VMEM((3, length * columns, channels), jnp.float32),
        ],
        compiler_params=pltpu.CompilerParams(vmem_limit_bytes=VMEM_LIMIT),
        cost_estimate=pl.CostEstimate(
            flops=2 * dots * columns * channels * channels,
            bytes_accessed=2 * TAPS * channels * channels,
            transcendentals=2 * length * columns * channels,
        ),
        name=body.__name__,
    )(*operands)


def place(ring, own, gathered, crossed, passed, crossed_passed):
    rows = own.shape[0]
    width = own.shape[1] // TAPS
    operands = [own, *gathered, *crossed, *passed, *crossed_passed]

    def body(*refs):
        own_ref, refs, out, sems = refs[0], refs[1:-2], refs[-2], refs[-1]
        index = lax.axis_index("ha")
        core = lax.rem(index, 2)
        side = lax.rem(index // 2, 2)
        turn = index // 4
        pair = lax.rem(lax.axis_index("grp"), 2)
        steps = len(gathered)
        copies = []

        def copy(source, row, column, span):
            if not isinstance(column, int):
                column = pl.multiple_of(column * width, 128)
            target = out.at[pl.ds(pl.multiple_of(row * rows, rows), rows), pl.ds(column, span * width)]
            one = pltpu.make_async_copy(source, target, sems.at[len(copies)])
            one.start()
            copies.append(one)

        copy(own_ref, 2 * turn + side, 0, TAPS)
        for step in range(steps):
            halves = []
            if step + 1 < steps:
                halves.append(2 * lax.rem(turn - step - 1 + ring, ring) + side)
            halves.append(2 * lax.rem(turn - step + ring, ring) + 1 - side)
            for place_at, row in enumerate(halves):
                part = pl.ds(place_at * rows, rows)
                first, second, third, fourth = (
                    refs[step],
                    refs[steps + step],
                    refs[2 * steps + step],
                    refs[3 * steps + step],
                )
                ours, theirs = (TAPS - SOLE) * pair, (TAPS - SOLE) * (1 - pair)
                copy(first.at[part, : HALF * width], row, ours + HALF * core, HALF)
                copy(first.at[part, HALF * width :], row, SOLE + (MID - 1) * core, MID)
                copy(second.at[part, : HALF * width], row, ours + HALF * (1 - core), HALF)
                skip = pl.multiple_of((HALF + 1 - core) * width, 128)
                copy(
                    second.at[part, pl.ds(skip, (MID - 1) * width)],
                    row,
                    SOLE + MID * (1 - core),
                    MID - 1,
                )
                copy(third.at[part], row, theirs + HALF * core, HALF)
                copy(fourth.at[part], row, theirs + HALF * (1 - core), HALF)
        for one in copies:
            one.wait()

    count = 1 + 6 * (2 * len(gathered) - 1)
    return pl.pallas_call(
        body,
        out_shape=jax.ShapeDtypeStruct((width, TAPS * width), own.dtype),
        in_specs=[pl.BlockSpec(memory_space=pltpu.HBM)] * len(operands),
        out_specs=pl.BlockSpec(memory_space=pltpu.VMEM),
        scratch_shapes=[pltpu.SemaphoreType.DMA((count,))],
        compiler_params=pltpu.CompilerParams(vmem_limit_bytes=VMEM_LIMIT),
        cost_estimate=pl.CostEstimate(
            flops=2 * 2**20, bytes_accessed=4 * TAPS * width * width, transcendentals=0
        ),
        name="place",
    )(*operands)


def gather(shards):
    count, groups = lax.axis_size("ha"), lax.axis_size("grp")
    rows, wide = shards[0].shape
    if count % 4 or groups % 2 or (2 * rows) % 16:
        return [lax.all_gather(shard, "ha", axis=0, tiled=True) for shard in shards]
    ring = count // 4
    width = wide // TAPS
    turns = [(i, (i + 4) % count) for i in range(count)]
    sides = [(i, i ^ 2) for i in range(count)]
    cores = [(i, i ^ 1) for i in range(count)]
    pairs = [(i, i ^ 1) for i in range(groups)]
    core = lax.axis_index("ha") % 2
    pair = lax.axis_index("grp") % 2
    kernels = []
    others = [lax.ppermute(shard, "ha", cores) for shard in shards]
    for shard, other in zip(shards, others):
        own = jnp.concatenate(
            [jnp.where(core == 0, shard, other), jnp.where(core == 0, other, shard)], axis=0
        )
        start = ((TAPS - SOLE) * pair + HALF * core) * width
        middle = (SOLE + (MID - 1) * core) * width
        piece = jnp.concatenate(
            [
                lax.dynamic_slice_in_dim(own, start, HALF * width, axis=1),
                lax.dynamic_slice_in_dim(own, middle, MID * width, axis=1),
            ],
            axis=1,
        )
        along = [piece]
        for _ in range(ring - 1):
            along.append(lax.ppermute(along[-1], "ha", turns))
        across = [lax.ppermute(block, "ha", sides) for block in along]
        gathered = [
            jnp.concatenate([along[step + 1], across[step]], axis=0) for step in range(ring - 1)
        ]
        gathered.append(across[-1])
        passed = [lax.ppermute(block[:, : HALF * width], "grp", pairs) for block in gathered]
        crossed = [lax.ppermute(block, "ha", cores) for block in gathered]
        crossed_passed = [lax.ppermute(block, "ha", cores) for block in passed]
        kernels.append(place(ring, own, gathered, crossed, passed, crossed_passed))
    return kernels


def neighbours(block):
    count = lax.axis_size("ha")
    forward = [(i, i + 1) for i in range(count - 1)]
    backward = [(i + 1, i) for i in range(count - 1)]
    return lax.ppermute(block, "ha", forward), lax.ppermute(block, "ha", backward)


def local(
    frames,
    cache_first,
    cache_second,
    gain_first,
    gain_second,
    bias_first,
    bias_second,
    weight_first,
    weight_second,
    cotangent,
):
    shape = frames.shape
    length, _, columns, channels = shape
    flat = (length, columns, channels)
    frames, cotangent = frames.reshape(flat), cotangent.reshape(flat)
    cache_first = cache_first.reshape(2, columns, channels)
    cache_second = cache_second.reshape(2, columns, channels)
    gain_first, gain_second, bias_first, bias_second = (
        v.reshape(1, channels) for v in (gain_first, gain_second, bias_first, bias_second)
    )
    low, high = neighbours(
        jnp.concatenate([cache_first, frames, cotangent, cache_second], axis=0)
    )
    kernel_one, kernel_two = gather([weight_first.T, weight_second.T])
    middle, act = run_kernel(
        first_kernel,
        length + 2,
        2,
        (cache_first, frames, low, high, gain_first, bias_first, gain_second, kernel_one),
        TAPS * length,
    )
    act_low, act_high = neighbours(act)
    grad = run_kernel(
        second_kernel,
        length,
        1,
        (cotangent, low, high, middle, gain_second, kernel_two),
        9 * (2 * length - 1),
    )
    grad_low, grad_high = neighbours(grad)
    out = run_kernel(
        third_kernel,
        length + 2,
        1,
        (cache_second, act, low, high, act_low, act_high, frames, bias_second, kernel_two),
        TAPS * length,
    )
    grad_frames = run_kernel(
        fourth_kernel,
        length,
        1,
        (grad, grad_low, grad_high, frames, gain_first, cotangent, kernel_one),
        9 * (2 * length - 1),
    )
    return out.reshape(shape), grad_frames.reshape(shape)


def solution(mesh):
    rows = P("grp", "ha", None, None)
    return jax.shard_map(
        local,
        mesh=mesh,
        in_specs=(rows, rows, rows, P(), P(), P(), P(), P(None, "ha"), P(None, "ha"), rows),
        out_specs=(rows, rows),
        check_vma=False,
    )
```

```python
import functools

import jax
import jax.numpy as jnp
from jax import lax
from jax.experimental import pallas as pl
from jax.experimental.pallas import tpu as pltpu
from jax.sharding import PartitionSpec as P


TILES = 81
SOLE = 32
HALF = SOLE // 2
MID = (TILES - 2 * SOLE + 1) // 2
VMEM_LIMIT = 12 * 1024 * 1024


def normed_silu(values, scales):
    mean_square = jnp.mean(values * values, axis=-1, keepdims=True)
    normed = values * lax.rsqrt(mean_square + 1e-06) * scales
    return normed * jax.nn.sigmoid(normed)


def silu_backward(values, scales, upstream):
    mean_square = jnp.mean(values * values, axis=-1, keepdims=True)
    inverse = lax.rsqrt(mean_square + 1e-06)
    normed = values * inverse * scales
    sigmoid_value = jax.nn.sigmoid(normed)
    scaled = scales * upstream * sigmoid_value * (1.0 + normed * (1.0 - sigmoid_value))
    return inverse * scaled - values * inverse**3 * jnp.mean(
        values * scaled, axis=-1, keepdims=True
    )


def shifted(block, by):
    zero = jnp.zeros_like(block[:, :1])
    if by > 0:
        return jnp.concatenate([zero, block[:, :-1]], axis=1)
    return jnp.concatenate([block[:, 1:], zero], axis=1)


def joined(parts_ref, length, columns, signs):
    parts = [parts_ref[k].reshape(length, columns, -1) for k in range(3)]
    return shifted(parts[0], signs) + parts[1] + shifted(parts[2], -signs)


def forward_dot(left, weight_ref, frame_tap, row_tap, col_tap):
    frames, columns, channels = left.shape
    start = (9 * frame_tap + 3 * row_tap + col_tap) * channels
    if not isinstance(start, int):
        start = pl.multiple_of(start, 128)
    return lax.dot_general(
        left.reshape(frames * columns, channels),
        weight_ref[:, pl.ds(start, channels)],
        (((1,), (1,)), ((), ())),
        preferred_element_type=jnp.float32,
    )


def backward_dot(left, weight_ref, frame_tap, row_tap, col_tap):
    frames, columns, channels = left.shape
    start = (9 * frame_tap + 3 * row_tap + col_tap) * channels
    if not isinstance(start, int):
        start = pl.multiple_of(start, 128)
    return lax.dot_general(
        left.reshape(frames * columns, channels),
        weight_ref[:, pl.ds(start, channels)],
        (((1,), (0,)), ((), ())),
        preferred_element_type=jnp.float32,
    )


def conv_forward(rows_ref, weight_ref, total_ref):
    length = rows_ref.shape[1] - 2
    for col_tap in range(3):
        for frame_tap in range(3):
            for row_tap in range(3):
                left = rows_ref[row_tap, frame_tap : frame_tap + length]
                product = forward_dot(left, weight_ref, frame_tap, row_tap, col_tap)
                if frame_tap == 0 and row_tap == 0:
                    total_ref[col_tap] = product
                else:
                    total_ref[col_tap] += product


def conv_backward(rows, weight_ref, total_ref, fresh):
    length, columns, _ = rows[0][1].shape
    for col_tap in range(3):
        start = fresh
        for row_tap, source in rows:
            for shift in range(min(3, length)):
                count = (length - shift) * columns
                product = backward_dot(source[shift:], weight_ref, 2 - shift, row_tap, col_tap)
                if start:
                    total_ref[col_tap] = product
                    start = False
                else:
                    total_ref[col_tap, :count] += product


def prepare_kernel(cache, frames, near, far, gain, rows):
    length = frames.shape[0]
    scales = gain[...][None, None]
    near_row, far_row = sides()
    for row, source in ((near_row, near), (1, None), (far_row, far)):
        rows[row, :2] = cache[...] if source is None else source[:2]
        values = frames[...] if source is None else source[2 : 2 + length]
        rows[row, 2:] = normed_silu(values.astype(jnp.float32), scales).astype(jnp.bfloat16)


def start_copies(pieces, sources, ring, weights, sems):
    width = weights[0].shape[1] // TILES
    copies = ([], [])
    for conv in range(2):
        for found in placements(pieces, sources, ring, width, conv):
            source, row, column, height, span = found
            target = weights[conv].at[pl.ds(row, height), pl.ds(column, span)]
            one = pltpu.make_async_copy(source, target, sems.at[conv, len(copies[conv])])
            one.start()
            copies[conv].append(one)
    return copies


def place_kernel(pieces, ring, *refs):
    sources, refs = refs[: len(pieces)], refs[-3:]
    copies = start_copies(pieces, sources, ring, refs[:2], refs[2])
    for one in copies[0] + copies[1]:
        one.wait()


def first_kernel(pieces, ring, rows, bias, gain, *refs):
    sources, refs = refs[: len(pieces)], refs[-6:]
    middle, act, weight_first, weight_second, total, sems = refs
    length, columns, _ = act.shape
    copies = start_copies(pieces, sources, ring, (weight_first, weight_second), sems)
    for one in copies[0]:
        one.wait()
    conv_forward(rows, weight_first, total)
    result = (joined(total, length, columns, 1) + bias[...][None, None]).astype(jnp.bfloat16)
    middle[...] = result
    act[...] = normed_silu(result.astype(jnp.float32), gain[...][None, None]).astype(jnp.bfloat16)
    for one in copies[1]:
        one.wait()


def second_kernel(cotangent, near, far, middle, gain, weight, grad, total):
    length, columns, _ = cotangent.shape
    span = slice(2 + length, 2 + 2 * length)
    near_row, far_row = sides()
    halo = ((1, cotangent[...]), (2 - near_row, near[span]), (2 - far_row, far[span]))
    conv_backward(halo, weight, total, True)
    upstream = joined(total, length, columns, -1)
    values = middle[...].astype(jnp.float32)
    grad[...] = silu_backward(values, gain[...][None, None], upstream).astype(jnp.bfloat16)


def third_kernel(
    cache, act, near, far, act_near, act_far, frames, bias, grad, weight_first, weight_second, *refs
):
    out, back_total, rows, total = refs
    length, columns, _ = act.shape
    past = slice(2 + 2 * length, 4 + 2 * length)
    near_row, far_row = sides()
    for row, older, newer in (
        (1, cache[...], act),
        (near_row, near[past], act_near),
        (far_row, far[past], act_far),
    ):
        rows[row, :2] = older
        rows[row, 2:] = newer[...]
    conv_backward(((1, grad[...]),), weight_first, back_total, True)
    conv_forward(rows, weight_second, total)
    result = joined(total, length, columns, 1) + bias[...][None, None]
    out[...] = (frames[...].astype(jnp.float32) + result).astype(jnp.bfloat16)


def fourth_kernel(near, far, frames, cotangent, gain, weight, total_in, grad_frames, total):
    length, columns, _ = frames.shape
    near_row, far_row = sides()
    total[...] = total_in[...]
    conv_backward(((2 - near_row, near[...]), (2 - far_row, far[...])), weight, total, False)
    upstream = joined(total, length, columns, -1)
    back = silu_backward(frames[...].astype(jnp.float32), gain[...][None, None], upstream)
    grad_frames[...] = (cotangent[...].astype(jnp.float32) + back).astype(jnp.bfloat16)


def call(body, outs, operands, flops, scratch=(), spaces=(), aliases=()):
    spec = pl.BlockSpec(memory_space=pltpu.VMEM)
    specs = [spec] * (len(operands) - len(spaces)) + list(spaces)
    return pl.pallas_call(
        body,
        out_shape=outs,
        in_specs=specs,
        out_specs=[spec] * len(outs),
        scratch_shapes=scratch,
        input_output_aliases=dict(aliases),
        compiler_params=pltpu.CompilerParams(vmem_limit_bytes=VMEM_LIMIT),
        cost_estimate=pl.CostEstimate(flops=flops, bytes_accessed=2**22, transcendentals=0),
    )(*operands)


def placements(pieces, sources, ring, width, conv):
    if ring == 0:
        return [(source, 0, 0, *source.shape) for source in sources[conv : conv + 1]]
    index = lax.axis_index("ha")
    core, side, turn = lax.rem(index, 2), lax.rem(index // 2, 2), index // 4
    pair = lax.rem(lax.axis_index("grp"), 2)
    found = []
    for (blocks, kind, crossed), source in zip(pieces, sources):
        whose = 1 - core if crossed else core
        for at, block in enumerate(blocks):
            block_conv, back, flip, height = block
            if block_conv != conv:
                continue
            chip = 2 * lax.rem(turn - back + ring, ring) + (1 - side if flip else side)
            begin = sum(b[3] for b in blocks[:at])
            part = pl.ds(begin, height)
            if kind == "own":
                column, span, skip = 0, TILES, 0
            elif kind == "middle" and not crossed:
                column, span, skip = SOLE + (MID - 1) * whose, MID, 0
            elif kind == "middle":
                column, span, skip = SOLE + MID * whose, MID - 1, whose
            else:
                where = 1 - pair if kind == "passed" else pair
                column, span, skip = (TILES - SOLE) * where + HALF * whose, HALF, 0
            if not isinstance(skip, int):
                skip = pl.multiple_of(skip * width, 128)
            if not isinstance(column, int):
                column = pl.multiple_of(column * width, 128)
            row = pl.multiple_of(chip * height, height)
            found.append(
                (source.at[part, pl.ds(skip, span * width)], row, column, height, span * width)
            )
    return found


def gather(shards):
    count, groups = lax.axis_size("ha"), lax.axis_size("grp")
    rows, wide = shards[0].shape
    if count % 4 or groups % 2 or (2 * rows) % 16:
        whole = [lax.all_gather(shard, "ha", axis=0, tiled=True) for shard in shards]
        return whole, [None, None], 0, [0, 0]
    ring = count // 4
    width = wide // TILES
    chip = 2 * rows

    turn = lambda a: lax.ppermute(a, "ha", [(i, (i + 4) % count) for i in range(count)])
    side = lambda a: lax.ppermute(a, "ha", [(i, i ^ 2) for i in range(count)])
    cross = lambda a: lax.ppermute(a, "ha", [(i, i ^ 1) for i in range(count)])
    over = lambda a: lax.ppermute(a, "grp", [(i, i ^ 1) for i in range(groups)])
    core = lax.axis_index("ha") % 2
    pair = lax.axis_index("grp") % 2
    others = [cross(shard) for shard in shards]

    own = [
        jnp.concatenate([jnp.where(core == 0, a, b), jnp.where(core == 0, b, a)], axis=0)
        for a, b in zip(shards, others)
    ]

    def chosen(start, taps):
        return jnp.concatenate(
            [lax.dynamic_slice_in_dim(o, start * width, taps * width, axis=1) for o in own], axis=0
        )

    ends = chosen((TILES - SOLE) * pair + HALF * core, HALF)
    mids = chosen(SOLE + (MID - 1) * core, MID)
    arrays, pieces, stages = [], [], []

    def keep(array, blocks, kind, stage):
        arrays.append(array)
        pieces.append((blocks, kind, False))
        arrays.append(cross(array))
        pieces.append((blocks, kind, True))
        stages.extend([stage, stage])

    ends_across = side(ends)
    ends_next = turn(ends)
    mids_across = side(mids)
    for conv in range(2):
        arrays.append(own[conv])
        pieces.append(([(conv, 0, False, chip)], "own", False))
        stages.append(0)
    keep(mids_across, [(0, 0, True, chip), (1, 0, True, chip)], "middle", 0)
    mids = jnp.concatenate([mids, mids_across], axis=0)
    for step in range(1, ring + 1):
        blocks = [(0, step - 1, True, chip), (1, step - 1, True, chip)]
        both = ends_across
        if step < ring:
            ends = ends_next
            blocks = [(0, step, False, chip), (1, step, False, chip)] + blocks
            both = jnp.concatenate([ends, ends_across], axis=0)
        keep(both, blocks, "ends", step)
        keep(over(both), blocks, "passed", step + 1)
        if step < ring:
            ends_across = side(ends)
            if step + 1 < ring:
                ends_next = turn(ends)
            mids = turn(mids)
            chips = [(conv, step, flip, chip) for flip in (False, True) for conv in range(2)]
            keep(mids, chips, "middle", step + 1)
    groups = [(stage > ring // 2) + (stage > ring) for stage in stages]
    return arrays, pieces, ring, groups


def neighbours(block):
    count = lax.axis_size("ha")
    inner = [(i, i ^ 1) for i in range(count)]
    outer = [(i, i + 1) for i in range(1, count - 1, 2)]
    outer += [(target, source) for source, target in outer]
    near = lax.ppermute(block, "ha", inner)
    far = lax.ppermute(block, "ha", outer)
    return near, far


def sides():
    core = lax.rem(lax.axis_index("ha"), 2)
    return 2 * (1 - core), 2 * core


def local(
    frames,
    cache_first,
    cache_second,
    gain_first,
    gain_second,
    bias_first,
    bias_second,
    weight_first,
    weight_second,
    cotangent,
):
    shape = frames.shape
    length, _, columns, channels = shape
    flat = (length, columns, channels)
    frames, cotangent = frames.reshape(flat), cotangent.reshape(flat)
    cache_first = cache_first.reshape(2, columns, channels)
    cache_second = cache_second.reshape(2, columns, channels)
    near, far = neighbours(jnp.concatenate([cache_first, frames, cotangent, cache_second], axis=0))
    arrays, pieces, ring, groups = gather([weight_first.T, weight_second.T])
    shape_of = lambda *dims: jax.ShapeDtypeStruct(dims, jnp.bfloat16)
    unit = 2 * columns * channels * channels
    totals = (3, length * columns, channels)
    total_of = jax.ShapeDtypeStruct(totals, jnp.float32)
    (rows,) = call(
        prepare_kernel,
        [shape_of(3, length + 2, columns, channels)],
        (cache_first, frames, near, far, gain_first),
        unit,
    )
    whole = [pltpu.VMEM((channels, 27 * channels), jnp.bfloat16)] * 2
    in_hbm = pl.BlockSpec(memory_space=pltpu.HBM)
    in_vmem = pl.BlockSpec(memory_space=pltpu.VMEM)
    kernels = []
    for group in range(2):
        these = [at for at in range(len(arrays)) if groups[at] == group]
        if not these:
            continue
        kernels = call(
            functools.partial(place_kernel, [pieces[at] for at in these], ring),
            whole,
            [arrays[at] for at in these] + kernels,
            unit * 9,
            [pltpu.SemaphoreType.DMA((2, 4 * len(these)))],
            [in_hbm] * len(these) + [in_vmem] * len(kernels),
            [(len(these) + at, at) for at in range(len(kernels))],
        )
        kernels = [pltpu.with_memory_space_constraint(k, pltpu.VMEM) for k in kernels]
    rest = [at for at in range(len(arrays)) if groups[at] == 2]
    scratch = pltpu.VMEM(totals, jnp.float32)
    middle, act, kernel_one, kernel_two = call(
        functools.partial(first_kernel, [pieces[at] for at in rest], ring),
        [shape_of(*flat)] * 2 + whole,
        (rows, bias_first, gain_second, *[arrays[at] for at in rest], *kernels),
        unit * 27 * length,
        [scratch, pltpu.SemaphoreType.DMA((2, 4 * len(arrays)))],
        [in_hbm] * len(rest) + [in_vmem] * 2,
        ((3 + len(rest), 2), (4 + len(rest), 3)),
    )
    kernel_one, kernel_two = (
        pltpu.with_memory_space_constraint(k, pltpu.VMEM) for k in (kernel_one, kernel_two)
    )
    act_near, act_far = neighbours(act)
    (grad,) = call(
        second_kernel,
        [shape_of(*flat)],
        (cotangent, near, far, middle, gain_second, kernel_two),
        unit * 9 * (2 * length - 1),
        [scratch],
    )
    grad_near, grad_far = neighbours(grad)
    out, back_total = call(
        third_kernel,
        [shape_of(*flat), total_of],
        (
            cache_second,
            act,
            near,
            far,
            act_near,
            act_far,
            frames,
            bias_second,
            grad,
            kernel_one,
            kernel_two,
        ),
        unit * 30 * length,
        [pltpu.VMEM((3, length + 2, columns, channels), jnp.bfloat16), scratch],
    )
    (grad_frames,) = call(
        fourth_kernel,
        [shape_of(*flat)],
        (grad_near, grad_far, frames, cotangent, gain_first, kernel_one, back_total),
        unit * 6 * (2 * length - 1),
        [scratch],
    )
    return out.reshape(shape), grad_frames.reshape(shape)


def solution(mesh):
    rows = P("grp", "ha", None, None)

    return jax.shard_map(
        local,
        mesh=mesh,
        in_specs=(rows, rows, rows, P(), P(), P(), P(), P(None, "ha"), P(None, "ha"), rows),
        out_specs=(rows, rows),
        check_vma=False,
    )
```

```python
import functools

import jax
import jax.numpy as jnp
from jax import lax
from jax.experimental import pallas as pl
from jax.experimental.pallas import tpu as pltpu
from jax.sharding import PartitionSpec as P


TILES = 81
SOLE = 32
VMEM_LIMIT = 12 * 1024 * 1024


def normed_silu(values, scales):
    mean_square = jnp.mean(values * values, axis=-1, keepdims=True)
    normed = values * lax.rsqrt(mean_square + 1e-06) * scales
    return normed * jax.nn.sigmoid(normed)


def silu_backward(values, scales, upstream):
    mean_square = jnp.mean(values * values, axis=-1, keepdims=True)
    inverse = lax.rsqrt(mean_square + 1e-06)
    normed = values * inverse * scales
    sigmoid_value = jax.nn.sigmoid(normed)
    scaled = scales * upstream * sigmoid_value * (1.0 + normed * (1.0 - sigmoid_value))
    return inverse * scaled - values * inverse**3 * jnp.mean(
        values * scaled, axis=-1, keepdims=True
    )


def shifted(block, by):
    zero = jnp.zeros_like(block[:, :1])
    if by > 0:
        return jnp.concatenate([zero, block[:, :-1]], axis=1)
    return jnp.concatenate([block[:, 1:], zero], axis=1)


def joined(parts_ref, length, columns, signs):
    parts = [parts_ref[k].reshape(length, columns, -1) for k in range(3)]
    return shifted(parts[0], signs) + parts[1] + shifted(parts[2], -signs)


def forward_dot(left, weight_ref, frame_tap, row_tap, col_tap):
    frames, columns, channels = left.shape
    start = (9 * frame_tap + 3 * row_tap + col_tap) * channels
    if not isinstance(start, int):
        start = pl.multiple_of(start, 128)
    return lax.dot_general(
        left.reshape(frames * columns, channels),
        weight_ref[:, pl.ds(start, channels)],
        (((1,), (1,)), ((), ())),
        preferred_element_type=jnp.float32,
    )


def backward_dot(left, weight_ref, frame_tap, row_tap, col_tap):
    frames, columns, channels = left.shape
    start = (9 * frame_tap + 3 * row_tap + col_tap) * channels
    if not isinstance(start, int):
        start = pl.multiple_of(start, 128)
    return lax.dot_general(
        left.reshape(frames * columns, channels),
        weight_ref[:, pl.ds(start, channels)],
        (((1,), (0,)), ((), ())),
        preferred_element_type=jnp.float32,
    )


def conv_forward(rows_ref, weight_ref, total_ref):
    length = rows_ref.shape[1] - 2
    for col_tap in range(3):
        for frame_tap in range(3):
            for row_tap in range(3):
                left = rows_ref[row_tap, frame_tap : frame_tap + length]
                product = forward_dot(left, weight_ref, frame_tap, row_tap, col_tap)
                if frame_tap == 0 and row_tap == 0:
                    total_ref[col_tap] = product
                else:
                    total_ref[col_tap] += product


def conv_backward(rows, weight_ref, total_ref, fresh):
    length, columns, _ = rows[0][1].shape
    for col_tap in range(3):
        start = fresh
        for row_tap, source in rows:
            for shift in range(min(3, length)):
                count = (length - shift) * columns
                product = backward_dot(source[shift:], weight_ref, 2 - shift, row_tap, col_tap)
                if start:
                    total_ref[col_tap] = product
                    start = False
                else:
                    total_ref[col_tap, :count] += product


def prepare_kernel(cache, frames, near, far, gain, rows):
    length = frames.shape[0]
    scales = gain[...][None, None]
    near_row, far_row = sides()
    for row, source in ((near_row, near), (1, None), (far_row, far)):
        rows[row, :2] = cache[...] if source is None else source[:2]
        values = frames[...] if source is None else source[2 : 2 + length]
        rows[row, 2:] = normed_silu(values.astype(jnp.float32), scales).astype(jnp.bfloat16)


def start_copies(pieces, sources, ring, weights, sems):
    width = weights[0].shape[1] // TILES
    copies = ([], [])
    for conv in range(2):
        for found in placements(pieces, sources, ring, width, conv):
            source, row, column, height, span = found
            target = weights[conv].at[pl.ds(row, height), pl.ds(column, span)]
            one = pltpu.make_async_copy(source, target, sems.at[conv, len(copies[conv])])
            one.start()
            copies[conv].append(one)
    return copies


def place_kernel(pieces, ring, *refs):
    sources, refs = refs[: len(pieces)], refs[-3:]
    copies = start_copies(pieces, sources, ring, refs[:2], refs[2])
    for one in copies[0] + copies[1]:
        one.wait()


def first_kernel(pieces, ring, rows, bias, gain, *refs):
    sources, refs = refs[: len(pieces)], refs[-6:]
    middle, act, weight_first, weight_second, total, sems = refs
    length, columns, _ = act.shape
    copies = start_copies(pieces, sources, ring, (weight_first, weight_second), sems)
    for one in copies[0]:
        one.wait()
    conv_forward(rows, weight_first, total)
    result = (joined(total, length, columns, 1) + bias[...][None, None]).astype(jnp.bfloat16)
    middle[...] = result
    act[...] = normed_silu(result.astype(jnp.float32), gain[...][None, None]).astype(jnp.bfloat16)
    for one in copies[1]:
        one.wait()


def second_kernel(cotangent, near, far, middle, gain, weight, grad, total):
    length, columns, _ = cotangent.shape
    span = slice(2 + length, 2 + 2 * length)
    near_row, far_row = sides()
    halo = ((1, cotangent[...]), (2 - near_row, near[span]), (2 - far_row, far[span]))
    conv_backward(halo, weight, total, True)
    upstream = joined(total, length, columns, -1)
    values = middle[...].astype(jnp.float32)
    grad[...] = silu_backward(values, gain[...][None, None], upstream).astype(jnp.bfloat16)


def third_kernel(
    cache, act, near, far, act_near, act_far, frames, bias, grad, weight_first, weight_second, *refs
):
    out, back_total, rows, total = refs
    length, columns, _ = act.shape
    past = slice(2 + 2 * length, 4 + 2 * length)
    near_row, far_row = sides()
    for row, older, newer in (
        (1, cache[...], act),
        (near_row, near[past], act_near),
        (far_row, far[past], act_far),
    ):
        rows[row, :2] = older
        rows[row, 2:] = newer[...]
    conv_backward(((1, grad[...]),), weight_first, back_total, True)
    conv_forward(rows, weight_second, total)
    result = joined(total, length, columns, 1) + bias[...][None, None]
    out[...] = (frames[...].astype(jnp.float32) + result).astype(jnp.bfloat16)


def fourth_kernel(near, far, frames, cotangent, gain, weight, total_in, grad_frames, total):
    length, columns, _ = frames.shape
    near_row, far_row = sides()
    total[...] = total_in[...]
    conv_backward(((2 - near_row, near[...]), (2 - far_row, far[...])), weight, total, False)
    upstream = joined(total, length, columns, -1)
    back = silu_backward(frames[...].astype(jnp.float32), gain[...][None, None], upstream)
    grad_frames[...] = (cotangent[...].astype(jnp.float32) + back).astype(jnp.bfloat16)


def call(body, outs, operands, flops, scratch=(), spaces=(), aliases=()):
    spec = pl.BlockSpec(memory_space=pltpu.VMEM)
    specs = [spec] * (len(operands) - len(spaces)) + list(spaces)
    return pl.pallas_call(
        body,
        out_shape=outs,
        in_specs=specs,
        out_specs=[spec] * len(outs),
        scratch_shapes=scratch,
        input_output_aliases=dict(aliases),
        compiler_params=pltpu.CompilerParams(vmem_limit_bytes=VMEM_LIMIT),
        cost_estimate=pl.CostEstimate(flops=flops, bytes_accessed=2**22, transcendentals=0),
    )(*operands)


def placements(pieces, sources, ring, width, conv):
    if ring == 0:
        return [(source, 0, 0, *source.shape) for source in sources[conv : conv + 1]]
    index = lax.axis_index("ha")
    core, side, turn = lax.rem(index, 2), lax.rem(index // 2, 2), index // 4
    pair = lax.rem(lax.axis_index("grp"), 2)
    found = []
    for (blocks, kind, crossed), source in zip(pieces, sources):
        whose = 1 - core if crossed else core
        for at, block in enumerate(blocks):
            block_conv, back, flip, height = block
            if block_conv != conv:
                continue
            chip = 2 * lax.rem(turn - back + ring, ring) + (1 - side if flip else side)
            begin = sum(b[3] for b in blocks[:at])
            part = pl.ds(begin, height)
            if kind == "own":
                column, span = 0, TILES
            elif kind == "middle":
                column, span = SOLE * width, TILES - 2 * SOLE
            else:
                where = 1 - pair if kind == "passed" else pair
                column, span = pl.multiple_of((TILES - SOLE) * width * where, 128), SOLE
            row = pl.multiple_of((2 * chip + whose) * height, height)
            found.append(
                (source.at[part], row, column, height, span * width)
            )
    return found


def gather(shards):
    count, groups = lax.axis_size("ha"), lax.axis_size("grp")
    rows, wide = shards[0].shape
    if count % 4 or groups % 2 or rows % 8:
        whole = [lax.all_gather(shard, "ha", axis=0, tiled=True) for shard in shards]
        return whole, [None, None], 0, [0, 0]
    ring = count // 4
    width = wide // TILES

    turn = lambda a: lax.ppermute(a, "ha", [(i, (i + 4) % count) for i in range(count)])
    side = lambda a: lax.ppermute(a, "ha", [(i, i ^ 2) for i in range(count)])
    cross = lambda a: lax.ppermute(a, "ha", [(i, i ^ 1) for i in range(count)])
    over = lambda a: lax.ppermute(a, "grp", [(i, i ^ 1) for i in range(groups)])
    pair = lax.axis_index("grp") % 2
    ends = jnp.concatenate(
        [
            lax.dynamic_slice_in_dim(v, (TILES - SOLE) * pair * width, SOLE * width, axis=1)
            for v in shards
        ],
        axis=0,
    )
    mids = jnp.concatenate([v[:, SOLE * width : (TILES - SOLE) * width] for v in shards], axis=0)
    arrays, pieces, stages = [], [], []

    def keep(array, blocks, kind, stage):
        arrays.append(array)
        pieces.append((blocks, kind, False))
        arrays.append(cross(array))
        pieces.append((blocks, kind, True))
        stages.extend([stage, stage])

    ends_across = side(ends)
    ends_next = turn(ends)
    mids_across = side(mids)
    for conv in range(2):
        keep(shards[conv], [(conv, 0, False, rows)], "own", 0)
    keep(mids_across, [(0, 0, True, rows), (1, 0, True, rows)], "middle", 0)
    mids = jnp.concatenate([mids, mids_across], axis=0)
    for step in range(1, ring + 1):
        blocks = [(0, step - 1, True, rows), (1, step - 1, True, rows)]
        both = ends_across
        if step < ring:
            ends = ends_next
            blocks = [(0, step, False, rows), (1, step, False, rows)] + blocks
            both = jnp.concatenate([ends, ends_across], axis=0)
        keep(both, blocks, "ends", step)
        keep(over(both), blocks, "passed", step + 1)
        if step < ring:
            ends_across = side(ends)
            if step + 1 < ring:
                ends_next = turn(ends)
            mids = turn(mids)
            chips = [(conv, step, flip, rows) for flip in (False, True) for conv in range(2)]
            keep(mids, chips, "middle", step + 1)
    groups = [(stage >= ring) + (stage > ring) for stage in stages]
    return arrays, pieces, ring, groups


def neighbours(block):
    count = lax.axis_size("ha")
    inner = [(i, i ^ 1) for i in range(count)]
    outer = [(i, i + 1) for i in range(1, count - 1, 2)]
    outer += [(target, source) for source, target in outer]
    near = lax.ppermute(block, "ha", inner)
    far = lax.ppermute(block, "ha", outer)
    return near, far


def sides():
    core = lax.rem(lax.axis_index("ha"), 2)
    return 2 * (1 - core), 2 * core


def local(
    frames,
    cache_first,
    cache_second,
    gain_first,
    gain_second,
    bias_first,
    bias_second,
    weight_first,
    weight_second,
    cotangent,
):
    shape = frames.shape
    length, _, columns, channels = shape
    flat = (length, columns, channels)
    frames, cotangent = frames.reshape(flat), cotangent.reshape(flat)
    cache_first = cache_first.reshape(2, columns, channels)
    cache_second = cache_second.reshape(2, columns, channels)
    near, far = neighbours(jnp.concatenate([cache_first, frames, cotangent, cache_second], axis=0))
    arrays, pieces, ring, groups = gather([weight_first.T, weight_second.T])
    shape_of = lambda *dims: jax.ShapeDtypeStruct(dims, jnp.bfloat16)
    unit = 2 * columns * channels * channels
    totals = (3, length * columns, channels)
    total_of = jax.ShapeDtypeStruct(totals, jnp.float32)
    (rows,) = call(
        prepare_kernel,
        [shape_of(3, length + 2, columns, channels)],
        (cache_first, frames, near, far, gain_first),
        unit,
    )
    whole = [pltpu.VMEM((channels, 27 * channels), jnp.bfloat16)] * 2
    in_hbm = pl.BlockSpec(memory_space=pltpu.HBM)
    in_vmem = pl.BlockSpec(memory_space=pltpu.VMEM)
    kernels = []
    for group in range(2):
        these = [at for at in range(len(arrays)) if groups[at] == group]
        if not these:
            continue
        kernels = call(
            functools.partial(place_kernel, [pieces[at] for at in these], ring),
            whole,
            [arrays[at] for at in these] + kernels,
            unit * 9,
            [pltpu.SemaphoreType.DMA((2, 4 * len(these)))],
            [in_hbm] * len(these) + [in_vmem] * len(kernels),
            [(len(these) + at, at) for at in range(len(kernels))],
        )
        kernels = [pltpu.with_memory_space_constraint(k, pltpu.VMEM) for k in kernels]
    rest = [at for at in range(len(arrays)) if groups[at] == 2]
    scratch = pltpu.VMEM(totals, jnp.float32)
    middle, act, kernel_one, kernel_two = call(
        functools.partial(first_kernel, [pieces[at] for at in rest], ring),
        [shape_of(*flat)] * 2 + whole,
        (rows, bias_first, gain_second, *[arrays[at] for at in rest], *kernels),
        unit * 27 * length,
        [scratch, pltpu.SemaphoreType.DMA((2, 4 * len(arrays)))],
        [in_hbm] * len(rest) + [in_vmem] * 2,
        ((3 + len(rest), 2), (4 + len(rest), 3)),
    )
    kernel_one, kernel_two = (
        pltpu.with_memory_space_constraint(k, pltpu.VMEM) for k in (kernel_one, kernel_two)
    )
    act_near, act_far = neighbours(act)
    (grad,) = call(
        second_kernel,
        [shape_of(*flat)],
        (cotangent, near, far, middle, gain_second, kernel_two),
        unit * 9 * (2 * length - 1),
        [scratch],
    )
    grad_near, grad_far = neighbours(grad)
    out, back_total = call(
        third_kernel,
        [shape_of(*flat), total_of],
        (
            cache_second,
            act,
            near,
            far,
            act_near,
            act_far,
            frames,
            bias_second,
            grad,
            kernel_one,
            kernel_two,
        ),
        unit * 30 * length,
        [pltpu.VMEM((3, length + 2, columns, channels), jnp.bfloat16), scratch],
    )
    (grad_frames,) = call(
        fourth_kernel,
        [shape_of(*flat)],
        (grad_near, grad_far, frames, cotangent, gain_first, kernel_one, back_total),
        unit * 6 * (2 * length - 1),
        [scratch],
    )
    return out.reshape(shape), grad_frames.reshape(shape)


def solution(mesh):
    rows = P("grp", "ha", None, None)

    return jax.shard_map(
        local,
        mesh=mesh,
        in_specs=(rows, rows, rows, P(), P(), P(), P(), P(None, "ha"), P(None, "ha"), rows),
        out_specs=(rows, rows),
        check_vma=False,
    )
```
